32 devices in a mesh: seq: 8 (over z, x), head: 4 (over y, core).
Axes of the slice: x: 2, y: 2, z: 4, core: 2. Of those that a mesh axis runs over, the one named last changes fastest.
Arguments:
- inputs: bfloat16 [2048, 3072], P('seq'), may hold values from -6 to 6
- decay_logs: float32 [12, 2048], P('head', 'seq'), may hold values from -3 to 0
- query_retain: bfloat16 [3072, 1536], P('seq', 'head'), may hold values from -0.109375 to 0.109375
- key_retain: bfloat16 [3072, 1536], P('seq', 'head'), may hold values from -0.109375 to 0.109375
- value_retain: bfloat16 [3072, 1536], P('seq', 'head'), may hold values from -0.109375 to 0.109375
- output_retain: bfloat16 [3072, 1536], P('seq', 'head'), may hold values from -0.15625 to 0.15625
- key_global: bfloat16 [3072, 512], P('seq', 'head')
- value_global: bfloat16 [3072, 512], P('seq', 'head'), may hold values from -0.109375 to 0.109375
- query_cross: bfloat16 [3072, 1536], P('seq', 'head')
Outputs:
- decoded: float32 [2048, 3072], P('seq')
- attended: bfloat16 [2048, 1536], P('seq', 'head')
The draws below stay inside these ranges and needn't reach their ends.
All inputs are finite; a program needn't handle non-finite values.
Results may differ from the reference program's by a relative error of at most 0.028.
Values may be sent and summed in bfloat16 or wider, within the bound.
A program may use at most 192 MiB of HBM per device.

```python
import jax
import jax.numpy as jnp
from jax import lax

D = 3072
HD = 128
H_RET = 12
KV_HEADS = 4
Q_CROSS = 12
TOK_DEV = 256
TOKENS = 2048
N_SEQ = 8
N_HEAD = 4


def cross_pair(key):
    asker_generator_init = jax.random.fold_in(key, 101)
    noise_seed = jax.random.fold_in(key, 102)
    queries = jax.random.normal(asker_generator_init, (D, Q_CROSS * HD), jnp.float32) * D ** (-0.5)
    fresh = jax.random.normal(noise_seed, (D, KV_HEADS * HD), jnp.float32) * D ** (-0.5)
    lookup_feature_width = fresh
    return (queries, lookup_feature_width)


def draw_query_cross(key, part):
    return cross_pair(key)[0].astype(jnp.bfloat16)


def draw_key_global(key, part):
    return cross_pair(key)[1].astype(jnp.bfloat16)


def draw_decay_logs(key, part):
    slow_share = 0.5
    slow_mask = jax.random.uniform(jax.random.fold_in(key, 201), (H_RET,), jnp.float32) < slow_share
    slow_rate = jax.random.uniform(jax.random.fold_in(key, 202), (H_RET,), jnp.float32, 0.1, 0.6) / TOKENS
    quick_decay_speed = jax.random.uniform(jax.random.fold_in(key, 203), (H_RET,), jnp.float32, 5.0, 9.0) / TOK_DEV
    decay_rate = jnp.where(slow_mask, slow_rate, quick_decay_speed)
    factor = jnp.exp(jax.random.uniform(jax.random.fold_in(key, 204), (H_RET, TOKENS // TOK_DEV), jnp.float32, jnp.log(0.5), jnp.log(2.0)))
    factor = jnp.repeat(factor, TOK_DEV, axis=1)
    jitter = jax.random.uniform(jax.random.fold_in(key, 205), (H_RET, TOKENS), jnp.float32, 0.5, 1.5)
    settled_period = -decay_rate[:, None] * factor * jitter
    placement_spots = jax.random.randint(jax.random.fold_in(key, 206), (H_RET, 2), 0, TOKENS)
    objective_history = jax.random.uniform(jax.random.fold_in(key, 207), (H_RET, 2), jnp.float32, 0.2, 0.5)
    position = jnp.arange(TOKENS, dtype=jnp.int32)
    agreement_number = (position[None, None, :] == placement_spots[:, :, None]).astype(jnp.float32)
    clustered_bunches = jnp.sum(agreement_number * jnp.log(1.0 - objective_history)[:, :, None], axis=1)
    return jnp.maximum(settled_period + clustered_bunches, -3.0)


def levels(key, dims, shards, smallest, high):
    factor_of, own = 1.0, jax.random.fold_in(key, 6)
    for dim, blocks in shards:
        steps = jnp.exp(jax.random.uniform(jax.random.fold_in(own, dim), (blocks,), jnp.float32, smallest / len(shards), high / len(shards)))
        factor_of = factor_of * jnp.repeat(steps, dims[dim] // blocks).reshape([-1 if axis == dim else 1 for axis in range(len(dims))])
    return factor_of


def gaussian(rng, shape, deviation, bound, pieces=(), kind=jnp.bfloat16):
    array = deviation * jax.random.normal(rng, shape, jnp.float32)
    if pieces:
        array = array * levels(rng, shape, pieces, -0.22, 0.18)
    return jnp.clip(array, -bound, bound).astype(kind)


def setup_inputs(seed: int = 0) -> dict:
    arg_keys = jax.random.split(jax.random.key(seed), 10)
    inputs = gaussian(arg_keys[0], (TOKENS, D), 1.0, 6.0, ((0, 8),))
    decay_logs = draw_decay_logs(jax.random.fold_in(arg_keys[9], 71), 0)
    query_retain = gaussian(arg_keys[2], (D, H_RET * HD), D ** -0.5, 0.109375, ((0, 8), (1, 4)))
    key_retain = gaussian(arg_keys[3], (D, H_RET * HD), D ** -0.5, 0.109375, ((0, 8), (1, 4)))
    value_retain = gaussian(arg_keys[4], (D, H_RET * HD), D ** -0.5, 0.109375, ((0, 8), (1, 4)))
    output_retain = gaussian(arg_keys[5], (D, H_RET * HD), (H_RET * HD) ** -0.5, 0.15625, ((0, 8), (1, 4)))
    key_global = draw_key_global(jax.random.fold_in(arg_keys[9], 71), 0)
    value_global = gaussian(arg_keys[7], (D, KV_HEADS * HD), D ** -0.5, 0.109375, ((0, 8), (1, 4)))
    query_cross = draw_query_cross(jax.random.fold_in(arg_keys[9], 71), 0)
    return dict(inputs=inputs, decay_logs=decay_logs, query_retain=query_retain, key_retain=key_retain, value_retain=value_retain, output_retain=output_retain, key_global=key_global, value_global=value_global, query_cross=query_cross)


def row_norm(values):
    return values * lax.rsqrt(lax.optimization_barrier(jnp.mean(values * values, axis=-1, keepdims=True)) + 1e-06)

def retain_block(carried_state, block_items):
    query_block, key_block, value_block, decay_block = block_items
    running = jnp.cumsum(decay_block, axis=-1)
    length = running.shape[-1]
    causal = jnp.arange(length)[:, None] >= jnp.arange(length)[None, :]
    spread = jnp.where(causal[None], running[:, :, None] - running[:, None, :], 0.0)
    weights = jnp.where(causal[None], jnp.exp(spread), 0.0)
    scores = jnp.einsum('htd,hsd->hts', query_block.astype(jnp.float32), key_block.astype(jnp.float32))
    weighted = (scores * weights).astype(jnp.bfloat16)
    within_block = jnp.einsum('hts,hse->hte', weighted.astype(jnp.float32), value_block.astype(jnp.float32))
    carried = jnp.einsum('htd,hde->hte', query_block.astype(jnp.float32), carried_state, precision=lax.Precision.HIGHEST) * jnp.exp(running)[:, :, None]
    tail_decay = jnp.exp(running[:, -1:] - running)
    faded_keys = (key_block.astype(jnp.float32) * tail_decay[:, :, None]).astype(jnp.bfloat16)
    resident_state = jnp.einsum('htd,hte->hde', faded_keys.astype(jnp.float32), value_block.astype(jnp.float32))
    next_state = jnp.exp(running[:, -1])[:, None, None] * carried_state + resident_state
    return (next_state, within_block + carried)

def reference(inputs, decay_logs, query_retain, key_retain, value_retain, output_retain, key_global, value_global, query_cross):
    input_full = inputs.astype(jnp.float32)
    normed = row_norm(input_full).astype(jnp.bfloat16)

    def by_block(matrix):
        projected = jnp.dot(normed, matrix, preferred_element_type=jnp.float32).astype(jnp.bfloat16)
        return projected.reshape(N_SEQ, TOK_DEV, H_RET, HD).transpose(0, 2, 1, 3)
    decay_blocks = decay_logs.reshape(H_RET, N_SEQ, TOK_DEV).transpose(1, 0, 2)
    start_state = jnp.zeros((H_RET, HD, HD), jnp.float32)
    final_state, outputs = lax.scan(retain_block, start_state, (by_block(query_retain), by_block(key_retain), by_block(value_retain), decay_blocks))
    retained = row_norm(outputs).astype(jnp.bfloat16).transpose(0, 2, 1, 3).reshape(TOKENS, H_RET * HD)
    group_width = H_RET * HD // N_HEAD
    mixed = jnp.zeros((TOKENS, D), jnp.float32)
    for group_index in range(N_HEAD):
        lower = group_index * group_width
        term = jnp.dot(retained[:, lower:lower + group_width], output_retain[:, lower:lower + group_width].T, preferred_element_type=jnp.float32)
        rounded = lax.optimization_barrier(term.astype(jnp.bfloat16))
        mixed = mixed + rounded.astype(jnp.float32)
    decoded = input_full + mixed
    normed_two = row_norm(decoded).astype(jnp.bfloat16)
    key_rows = jnp.dot(normed_two, key_global, preferred_element_type=jnp.float32).astype(jnp.bfloat16)
    value_rows = jnp.dot(normed_two, value_global, preferred_element_type=jnp.float32).astype(jnp.bfloat16)
    cross_queries = (jnp.dot(normed_two, query_cross, preferred_element_type=jnp.float32) * HD ** (-0.5)).astype(jnp.bfloat16)
    group_size = Q_CROSS // KV_HEADS
    key_heads = key_rows.reshape(TOKENS, KV_HEADS, HD).astype(jnp.float32)
    value_heads = value_rows.reshape(TOKENS, KV_HEADS, HD).astype(jnp.float32)
    query_blocks = cross_queries.reshape(N_SEQ, TOK_DEV, KV_HEADS, group_size, HD)
    block_starts = jnp.arange(N_SEQ, dtype=jnp.int32) * TOK_DEV

    def attend(block_items):
        query_block, block_start = block_items
        scores = jnp.einsum('tgqd,sgd->gqts', query_block.astype(jnp.float32), key_heads)
        query_positions = block_start + jnp.arange(TOK_DEV, dtype=jnp.int32)
        allowed = jnp.arange(TOKENS, dtype=jnp.int32)[None, :] <= query_positions[:, None]
        masked = jnp.where(allowed, scores, -1e+30)
        row_top = lax.optimization_barrier(jnp.max(masked, axis=-1, keepdims=True))
        probabilities = jnp.where(allowed, jnp.exp(masked - row_top), 0.0)
        row_total = lax.optimization_barrier(jnp.sum(probabilities, axis=-1))
        rounded = lax.optimization_barrier(probabilities.astype(jnp.bfloat16))
        gathered = jnp.einsum('gqts,sgd->gqtd', rounded.astype(jnp.float32), value_heads)
        result = gathered / row_total[..., None]
        return result.transpose(2, 0, 1, 3).reshape(TOK_DEV, Q_CROSS * HD).astype(jnp.bfloat16)
    attended = lax.map(attend, (query_blocks, block_starts)).reshape(TOKENS, Q_CROSS * HD)
    return (decoded, attended)
```

```python
import functools

import jax
import jax.numpy as jnp
from jax import lax
from jax.experimental import pallas as pl
from jax.experimental.pallas import tpu as pltpu
from jax.sharding import PartitionSpec as P

HD = 128
F32 = jnp.float32
BF16 = jnp.bfloat16
MESH = pl.DeviceIdType.MESH
KEY, VALUE, QUERY, OUT, CROSS = range(5)


def dot(a, b, dims=((1,), (0,)), precision=None):
    return lax.dot_general(a, b, (dims, ((), ())), precision=precision, preferred_element_type=F32)


def kernel(
    n,
    x_ref, run_row_ref, run_col_ref, tot_ref,
    wk_ref, wv_ref, wq_ref, wo_ref, wc_ref,
    dec_ref, att_ref,
    gk, gv, gq, go, gc, tots, states, kvs,
    normed, q_buf, k_buf, v_buf, ret, part, got_a, pair, got_b, mine, got_c,
    q_rows, top, total, acc,
    w_send, w_recv, wx_send, w_local, t_send, t_recv,
    s_send, s_recv, sx_send, kv_send, kv_recv, kvx_send, h_send, h_recv,
):
    me = lax.axis_index("seq")
    head = lax.axis_index("head")
    rows, width = x_ref.shape
    heads = wq_ref.shape[1] // HD
    half_n = n // 2
    twin = me + 1 - 2 * lax.rem(me, 2)
    core = lax.rem(head, 2)
    near = head + 1 - 2 * core
    far = lax.rem(head + 2, 4)
    own_refs = (wk_ref, wv_ref, wq_ref, wo_ref, wc_ref)
    full_refs = (gk, gv, gq, go, gc)

    def peer(k):
        return lax.rem(me + 2 * k, n)

    def twin_peer(k):
        return lax.rem(twin + 2 * k, n)

    barrier = pltpu.get_barrier_semaphore()

    @pl.loop(0, n - 1)
    def _(k):
        pl.semaphore_signal(
            barrier, inc=1, device_id={"seq": lax.rem(me + 1 + k, n)}, device_id_type=MESH
        )

    for other in (near, far):
        pl.semaphore_signal(barrier, inc=1, device_id={"head": other}, device_id_type=MESH)
    pl.semaphore_wait(barrier, n + 1)

    def slot(m, o):
        depth = own_refs[m].shape[0]
        return full_refs[m].at[pl.ds(pl.multiple_of(o * depth, depth), depth), :]

    def z_copy(m, k):
        return pltpu.make_async_remote_copy(
            own_refs[m], slot(m, me), w_send.at[m, k], w_recv.at[m, me],
            device_id={"seq": peer(k)}, device_id_type=MESH)

    def own_to_twin(m):
        return pltpu.make_async_remote_copy(
            own_refs[m], slot(m, me), wx_send.at[m, 0], w_recv.at[m, me],
            device_id={"seq": twin}, device_id_type=MESH)

    def x_copy(m, k):
        o = peer(k)
        return pltpu.make_async_remote_copy(
            slot(m, o), slot(m, o), wx_send.at[m, k], w_recv.at[m, o],
            device_id={"seq": twin}, device_id_type=MESH)

    def w_arrival(m, o):
        return pltpu.make_async_remote_copy(
            slot(m, o), slot(m, o), wx_send.at[m, 0], w_recv.at[m, o],
            device_id={"seq": twin}, device_id_type=MESH)

    def local_copy(m):
        return pltpu.make_async_copy(own_refs[m], slot(m, me), w_local.at[m])

    def start_gather(m):
        own_to_twin(m).start()

        @pl.loop(1, half_n)
        def _(k):
            z_copy(m, k).start()

        local_copy(m).start()

    def forward(m):
        @pl.loop(1, half_n)
        def _(k):
            w_arrival(m, peer(k)).wait_recv()
            x_copy(m, k).start()

    def finish(m):
        @pl.loop(0, half_n)
        def _(k):
            w_arrival(m, twin_peer(k)).wait_recv()

        local_copy(m).wait()

    def finish_sends(m):
        own_to_twin(m).wait_send()

        @pl.loop(1, half_n)
        def _(k):
            z_copy(m, k).wait_send()
            x_copy(m, k).wait_send()

    def causal_ops(buf, send, recv, x_send):
        def direct(k):
            return pltpu.make_async_remote_copy(
                buf.at[me], buf.at[me], send.at[k], recv.at[me],
                device_id={"seq": me + 2 * k}, device_id_type=MESH)

        def across(o, k):
            return pltpu.make_async_remote_copy(
                buf.at[o], buf.at[o], x_send.at[k], recv.at[o],
                device_id={"seq": twin}, device_id_type=MESH)

        z = me // 2
        odd = lax.rem(me, 2)

        def start():
            @pl.when(odd == 0)
            def _():
                across(me, 0).start()

            @pl.loop(1, half_n - z)
            def _(k):
                direct(k).start()

        def relay():
            @pl.loop(1, z + 1)
            def _(k):
                o = me - 2 * k
                across(o, k).wait_recv()
                across(o, k).start()

        def finish():
            @pl.loop(0, z + odd)
            def _(k):
                across(me - 1 - 2 * k, 0).wait_recv()

        def finish_sends():
            @pl.when(odd == 0)
            def _():
                across(me, 0).wait_send()

            @pl.loop(1, half_n - z)
            def _(k):
                direct(k).wait_send()

            @pl.loop(1, z + 1)
            def _(k):
                across(me - 2 * k, k).wait_send()

        return start, relay, finish, finish_sends

    def total_copy(p):
        return pltpu.make_async_remote_copy(
            tot_ref, tots.at[me], t_send.at[p], t_recv.at[me],
            device_id={"seq": p}, device_id_type=MESH)

    @pl.loop(me + 1, n)
    def _(p):
        total_copy(p).start()

    start_gather(KEY)
    start_gather(VALUE)
    start_gather(QUERY)

    @pl.loop(0, rows // 32)
    def _(i):
        part_rows = pl.ds(i * 32, 32)
        x = x_ref[part_rows, :].astype(F32)
        normed[part_rows, :] = (
            x * lax.rsqrt(jnp.mean(x * x, axis=-1, keepdims=True) + 1e-06)).astype(BF16)

    forward(KEY)
    forward(VALUE)
    finish(KEY)
    k_buf[...] = dot(normed[...], gk[...]).astype(BF16)
    finish(VALUE)
    v_buf[...] = dot(normed[...], gv[...]).astype(BF16)
    for h in range(heads):
        cols = slice(h * HD, (h + 1) * HD)
        col = run_col_ref[:, h:h + 1]
        tail = jnp.exp(run_row_ref[h:h + 1, rows - 1:rows] - col)
        faded = (k_buf[:, cols].astype(F32) * tail).astype(BF16)
        states[me, cols, :] = dot(faded, v_buf[:, cols], ((0,), (0,))).astype(BF16)
    s_start, s_relay, s_finish, s_done = causal_ops(states, s_send, s_recv, sx_send)
    s_start()
    start_gather(OUT)
    start_gather(CROSS)

    forward(QUERY)
    finish(QUERY)
    q_buf[...] = dot(normed[...], gq[...]).astype(BF16)

    @pl.loop(0, me)
    def _(o):
        pltpu.make_async_remote_copy(
            tots.at[o], tots.at[o], t_send.at[o], t_recv.at[o],
            device_id={"seq": twin}, device_id_type=MESH).wait_recv()

    s_relay()
    s_finish()
    t_iota = lax.broadcasted_iota(jnp.int32, (rows, rows), 0)
    s_iota = lax.broadcasted_iota(jnp.int32, (rows, rows), 1)
    for h in range(heads):
        cols = slice(h * HD, (h + 1) * HD)
        col = run_col_ref[:, h:h + 1]
        causal = t_iota >= s_iota
        spread = jnp.where(causal, col - run_row_ref[h:h + 1, :], 0.0)
        decay = jnp.where(causal, jnp.exp(spread), 0.0)
        scores = dot(q_buf[:, cols], k_buf[:, cols], ((1,), (1,)))
        weighted = (scores * decay).astype(BF16)
        within = dot(weighted, v_buf[:, cols])

        def step(o, state):
            return jnp.exp(tots[o, h:h + 1, :]) * state + states[o, cols, :].astype(F32)

        incoming = lax.fori_loop(0, me, step, jnp.zeros((HD, HD), F32))
        carried = dot(
            q_buf[:, cols].astype(F32), incoming, precision=lax.Precision.HIGHEST) * jnp.exp(col)
        raw = within + carried
        ret[:, cols] = (
            raw * lax.rsqrt(jnp.mean(raw * raw, axis=-1, keepdims=True) + 1e-06)).astype(BF16)

    half = width // 2
    piece = half // 3

    def head_copy(src, dst, i, other):
        return pltpu.make_async_remote_copy(
            src, dst, h_send.at[i], h_recv.at[i], device_id={"head": other}, device_id_type=MESH)

    def project(side):
        for c in range(3):
            base = pl.multiple_of(side * half + c * piece, piece)
            term = dot(ret[...], go[pl.ds(base, piece), :], ((1,), (1,)))
            part[side, :, c * piece:(c + 1) * piece] = term.astype(BF16)

    forward(OUT)
    finish(OUT)
    project(1 - core)
    to_near = head_copy(part.at[1 - core], got_a, 0, near)
    to_near.start()
    project(core)
    to_near.wait_recv()
    pair[...] = (part[core].astype(F32) + got_a[...].astype(F32)).astype(BF16)
    to_far = head_copy(pair, got_b, 1, far)
    to_far.start()
    forward(CROSS)
    to_far.wait_recv()
    mine[...] = (pair[...].astype(F32) + got_b[...].astype(F32)).astype(BF16)
    back = head_copy(mine, got_c, 2, near)
    back.start()
    own_cols = pl.ds(pl.multiple_of(core * half, half), half)
    dec_ref[:, own_cols] = x_ref[:, own_cols].astype(F32) + mine[...].astype(F32)
    back.wait_recv()
    other_cols = pl.ds(pl.multiple_of((1 - core) * half, half), half)
    dec_ref[:, other_cols] = x_ref[:, other_cols].astype(F32) + got_c[...].astype(F32)

    @pl.loop(0, rows // 32)
    def _(i):
        part_rows = pl.ds(i * 32, 32)
        d = dec_ref[part_rows, :]
        normed[part_rows, :] = (
            d * lax.rsqrt(jnp.mean(d * d, axis=-1, keepdims=True) + 1e-06)).astype(BF16)

    finish(CROSS)
    kvs[me] = dot(normed[...], gc[:, :2 * HD]).astype(BF16)
    kv_start, kv_relay, kv_finish, kv_done = causal_ops(kvs, kv_send, kv_recv, kvx_send)
    kv_start()
    for g in range(heads):
        cols = slice((2 + g) * HD, (3 + g) * HD)
        q_rows[g * rows:(g + 1) * rows, :] = (dot(normed[...], gc[:, cols]) * HD ** -0.5).astype(BF16)

    for g in range(heads):
        block = slice(g * rows, (g + 1) * rows)
        scores = dot(q_rows[block, :], kvs[me, :, :HD], ((1,), (1,)))
        scores = jnp.where(t_iota >= s_iota, scores, -1e30)
        high = jnp.max(scores, axis=-1, keepdims=True)
        weights = jnp.exp(scores - high)
        top[block, :] = high
        total[block, :] = jnp.sum(weights, axis=-1, keepdims=True)
        acc[block, :] = dot(weights.astype(BF16), kvs[me, :, HD:])

    kv_relay()
    kv_finish()

    @pl.loop(0, me)
    def _(o):
        for g in range(heads):
            block = slice(g * rows, (g + 1) * rows)
            scores = dot(q_rows[block, :], kvs[o, :, :HD], ((1,), (1,)))
            old = top[block, :]
            high = jnp.maximum(old, jnp.max(scores, axis=-1, keepdims=True))
            weights = jnp.exp(scores - high)
            shrink = jnp.exp(old - high)
            top[block, :] = high
            total[block, :] = total[block, :] * shrink + jnp.sum(weights, axis=-1, keepdims=True)
            acc[block, :] = acc[block, :] * shrink + dot(weights.astype(BF16), kvs[o, :, HD:])

    for g in range(heads):
        block = slice(g * rows, (g + 1) * rows)
        att_ref[:, g * HD:(g + 1) * HD] = (acc[block, :] / total[block, :]).astype(BF16)

    @pl.loop(me + 1, n)
    def _(p):
        total_copy(p).wait_send()

    for m in range(5):
        finish_sends(m)
    s_done()
    kv_done()
    to_near.wait_send()
    to_far.wait_send()
    back.wait_send()


def body(n, inputs, decay_logs, wq, wk, wv, wo, kg, vg, qc):
    rows, width = inputs.shape
    inner = wq.shape[1]
    heads = inner // HD
    running = jnp.cumsum(decay_logs, axis=-1)
    run_row = jnp.pad(running, ((0, 8 - heads), (0, 0)))
    run_col = run_row.T
    totals = jnp.broadcast_to(run_row[:, -1:], (8, HD))
    wc = jnp.concatenate([kg, vg, qc], axis=1)
    vmem = pl.BlockSpec(memory_space=pltpu.VMEM)
    half = width // 2
    dma = pltpu.SemaphoreType.DMA
    half_n = n // 2
    return pl.pallas_call(
        functools.partial(kernel, n),
        out_shape=(
            jax.ShapeDtypeStruct((rows, width), F32),
            jax.ShapeDtypeStruct((rows, inner), BF16),
        ),
        in_specs=[vmem] * 9,
        out_specs=(vmem, vmem),
        scratch_shapes=[
            pltpu.VMEM((width, inner), BF16),
            pltpu.VMEM((width, inner), BF16),
            pltpu.VMEM((width, inner), BF16),
            pltpu.VMEM((width, inner), BF16),
            pltpu.VMEM((width, inner + 2 * HD), BF16),
            pltpu.VMEM((n, 8, HD), F32),
            pltpu.VMEM((n, inner, HD), BF16),
            pltpu.VMEM((n, rows, 2 * HD), BF16),
            pltpu.VMEM((rows, width), BF16),
            pltpu.VMEM((rows, inner), BF16),
            pltpu.VMEM((rows, inner), BF16),
            pltpu.VMEM((rows, inner), BF16),
            pltpu.VMEM((rows, inner), BF16),
            pltpu.VMEM((2, rows, half), BF16),
            pltpu.VMEM((rows, half), BF16),
            pltpu.VMEM((rows, half), BF16),
            pltpu.VMEM((rows, half), BF16),
            pltpu.VMEM((rows, half), BF16),
            pltpu.VMEM((rows, half), BF16),
            pltpu.VMEM((heads * rows, HD), BF16),
            pltpu.VMEM((heads * rows, 1), F32),
            pltpu.VMEM((heads * rows, 1), F32),
            pltpu.VMEM((heads * rows, HD), F32),
            dma((5, half_n)), dma((5, n)), dma((5, half_n)), dma((5,)),
            dma((n,)), dma((n,)),
            dma((half_n,)), dma((n,)), dma((half_n,)),
            dma((half_n,)), dma((n,)), dma((half_n,)),
            dma((3,)), dma((3,)),
        ],
        compiler_params=pltpu.CompilerParams(
            collective_id=0, has_side_effects=True, vmem_limit_bytes=60 * 1024 * 1024),
        name="layer",
    )(inputs, run_row, run_col, totals, wk, wv, wq, wo, wc)


def solution(mesh):
    n = mesh.shape["seq"]

    def run(*args):
        return body(n, *args)

    in_specs = (P("seq", None), P("head", "seq")) + (P("seq", "head"),) * 7
    out_specs = (P("seq", None), P("seq", "head"))
    return jax.shard_map(run, mesh=mesh, in_specs=in_specs, out_specs=out_specs, check_vma=False)
```

```python
import functools

import jax
import jax.numpy as jnp
from jax import lax
from jax.experimental import pallas as pl
from jax.experimental.pallas import tpu as pltpu
from jax.sharding import PartitionSpec as P

HD = 128
F32 = jnp.float32
BF16 = jnp.bfloat16
MESH = pl.DeviceIdType.MESH
KEY, VALUE, QUERY, OUT, CROSS, KEY_GLOBAL, VALUE_GLOBAL = range(7)
PLUS = (True, False, True, False, True, False, False)


def dot(a, b, dims=((1,), (0,)), precision=None):
    return lax.dot_general(a, b, (dims, ((), ())), precision=precision, preferred_element_type=F32)


def kernel(
    n, aligned,
    x_ref, xs_ref, run_row_ref, run_col_ref, tot_ref,
    wk_ref, wv_ref, wq_ref, wo_ref, wc_ref, wkg_ref, wvg_ref,
    dec_out, att_ref,
    gk, gv, gq, go, gc, gkg, gvg, tots, states, kvs,
    dec_ref, nx, twin_nx, sent, got, within_buf,
    normed, q_buf, k_buf, v_buf, ret, part, got_a, pair, got_b, mine, got_c,
    q_rows, top, total, acc,
    wp_send, wm_send, w_recv, wx_send, w_local, t_send, t_recv,
    s_send, s_recv, sx_send, kv_send, kv_recv, kvx_send, h_send, h_recv, p_send, p_recv, out_sem,
):
    me = lax.axis_index("seq")
    head = lax.axis_index("head")
    rows, width = x_ref.shape
    heads = wq_ref.shape[1] // HD
    half_n = n // 2
    mid = half_n // 2
    odd = lax.rem(me, 2)
    twin = me + 1 - 2 * odd
    core = lax.rem(head, 2)
    near = head + 1 - 2 * core
    far = lax.rem(head + 2, 4)
    own_refs = (wk_ref, wv_ref, wq_ref, wo_ref, wc_ref, wkg_ref, wvg_ref)
    full_refs = (gk, gv, gq, go, gc, gkg, gvg)
    up = lax.rem(me + 2, n)
    down = lax.rem(me + n - 2, n)

    barrier = pltpu.get_barrier_semaphore()

    @pl.loop(0, n - 1)
    def _(k):
        pl.semaphore_signal(
            barrier, inc=1, device_id={"seq": lax.rem(me + 1 + k, n)}, device_id_type=MESH
        )

    for other in (near, far):
        pl.semaphore_signal(barrier, inc=1, device_id={"head": other}, device_id_type=MESH)
    pl.semaphore_wait(barrier, n + 1)

    def slot(m, o):
        depth = own_refs[m].shape[0]
        place = o // 2 if m < OUT else o
        return full_refs[m].at[pl.ds(pl.multiple_of(place * depth, depth), depth), :]

    def ring_copy(m, s, plus):
        o = lax.rem(me + n - 2 * s, n) if plus else lax.rem(me + 2 * s, n)
        src = own_refs[m] if s == 0 else slot(m, o)
        return pltpu.make_async_remote_copy(
            src, slot(m, o), (wp_send if plus else wm_send).at[m, s], w_recv.at[m, o],
            device_id={"seq": up if plus else down}, device_id_type=MESH)

    def x_copy(m, o, own=False):
        return pltpu.make_async_remote_copy(
            own_refs[m] if own else slot(m, o), slot(m, o), wx_send.at[m, o // 2], w_recv.at[m, o],
            device_id={"seq": twin}, device_id_type=MESH)

    def local_copy(m):
        return pltpu.make_async_copy(own_refs[m], slot(m, me), w_local.at[m])

    def start_gather(m):
        ring_copy(m, 0, True).start()
        ring_copy(m, 0, False).start()
        if m >= OUT:
            x_copy(m, me, own=True).start()
        local_copy(m).start()

    def arrive(m, o):
        x_copy(m, o).wait_recv()

    def forward(m):
        for s in range(1, mid):
            for plus in (True, False):
                o = lax.rem(me + n - 2 * s, n) if plus else lax.rem(me + 2 * s, n)
                arrive(m, o)
                if s < mid - 1 or plus == PLUS[m]:
                    ring_copy(m, s, plus).start()
                if m >= OUT:
                    x_copy(m, o).start()

    def settle(m):
        o = lax.rem(me + 2 * mid, n)
        arrive(m, o)
        if m >= OUT:
            x_copy(m, o).start()
        local_copy(m).wait()

    def finish(m):
        @pl.loop(0, half_n)
        def _(k):
            arrive(m, lax.rem(twin + 2 * k, n))

    def finish_sends(m):
        for s in range(mid):
            for plus in (True, False):
                if s < mid - 1 or plus == PLUS[m]:
                    ring_copy(m, s, plus).wait_send()
        if m >= OUT:
            x_copy(m, me, own=True).wait_send()

            @pl.loop(1, half_n)
            def _(k):
                x_copy(m, lax.rem(me + 2 * k, n)).wait_send()

    z = me // 2

    def causal_ops(buf, send, recv, x_send):
        def direct(k):
            return pltpu.make_async_remote_copy(
                buf.at[me], buf.at[me], send.at[k], recv.at[me],
                device_id={"seq": me + 2 * k}, device_id_type=MESH)

        def across(o, k):
            return pltpu.make_async_remote_copy(
                buf.at[o], buf.at[o], x_send.at[k], recv.at[o],
                device_id={"seq": twin}, device_id_type=MESH)

        def start():
            @pl.when(odd == 0)
            def _():
                across(me, 0).start()

            @pl.loop(1, half_n - z)
            def _(k):
                direct(k).start()

        def relay(use=None):
            @pl.loop(1, z + 1)
            def _(k):
                o = me - 2 * k
                across(o, k).wait_recv()
                across(o, k).start()
                if use is not None:
                    use(o)

        def finish(use=None):
            @pl.loop(0, z + odd)
            def _(k):
                across(me - 1 - 2 * k, 0).wait_recv()
                if use is not None:
                    use(me - 1 - 2 * k)

        def finish_sends():
            @pl.when(odd == 0)
            def _():
                across(me, 0).wait_send()

            @pl.loop(1, half_n - z)
            def _(k):
                direct(k).wait_send()

            @pl.loop(1, z + 1)
            def _(k):
                across(me - 2 * k, k).wait_send()

        return start, relay, finish, finish_sends

    def total_copy(p):
        return pltpu.make_async_remote_copy(
            tot_ref, tots.at[me], t_send.at[p], t_recv.at[me],
            device_id={"seq": p}, device_id_type=MESH)

    @pl.loop(me + 1, n)
    def _(p):
        total_copy(p).start()

    start_gather(KEY)
    start_gather(VALUE)
    depth = wq_ref.shape[0]

    @pl.loop(0, rows // 32)
    def _(i):
        part_rows = pl.ds(i * 32, 32)
        x = x_ref[part_rows, :].astype(F32)
        scale = lax.rsqrt(jnp.mean(x * x, axis=-1, keepdims=True) + 1e-06)
        for side in range(2):
            if aligned:
                for j in range(half_n):
                    cols = slice((2 * j + side) * depth, (2 * j + side + 1) * depth)
                    nx[side, part_rows, j * depth:(j + 1) * depth] = (
                        x_ref[part_rows, cols].astype(F32) * scale).astype(BF16)
            else:
                nx[side, part_rows, :] = (
                    xs_ref[side, part_rows, :].astype(F32) * scale).astype(BF16)

    def twin_copy(src, dst, i):
        return pltpu.make_async_remote_copy(
            src, dst, p_send.at[i], p_recv.at[i], device_id={"seq": twin}, device_id_type=MESH)

    tokens = twin_copy(nx.at[1 - odd], twin_nx, 3)
    tokens.start()

    def share(m):
        twin_part = dot(twin_nx[...], full_refs[m][...])
        sent[m] = twin_part.astype(BF16)
        twin_copy(sent.at[m], got.at[m], m).start()
        return dot(nx[odd], full_refs[m][...])

    def combine(m, own, dst):
        twin_copy(sent.at[m], got.at[m], m).wait_recv()
        dst[...] = (own + got[m].astype(F32)).astype(BF16)

    forward(KEY)
    forward(VALUE)
    start_gather(QUERY)
    tokens.wait_recv()
    settle(KEY)
    within_buf[...] = share(KEY)
    settle(VALUE)
    value_part = share(VALUE)
    combine(KEY, within_buf[...], k_buf)
    combine(VALUE, value_part, v_buf)
    forward(QUERY)
    for h in range(heads):
        cols = slice(h * HD, (h + 1) * HD)
        col = run_col_ref[:, h:h + 1]
        tail = jnp.exp(run_row_ref[h:h + 1, rows - 1:rows] - col)
        faded = (k_buf[:, cols].astype(F32) * tail).astype(BF16)
        states[me, cols, :] = dot(faded, v_buf[:, cols], ((0,), (0,))).astype(BF16)
    s_start, s_relay, s_finish, s_done = causal_ops(states, s_send, s_recv, sx_send)
    s_start()
    start_gather(OUT)
    settle(QUERY)
    query_part = share(QUERY)
    combine(QUERY, query_part, q_buf)
    t_iota = lax.broadcasted_iota(jnp.int32, (rows, rows), 0)
    s_iota = lax.broadcasted_iota(jnp.int32, (rows, rows), 1)
    for h in range(heads):
        cols = slice(h * HD, (h + 1) * HD)
        col = run_col_ref[:, h:h + 1]
        causal = t_iota >= s_iota
        spread = jnp.where(causal, col - run_row_ref[h:h + 1, :], 0.0)
        decay = jnp.where(causal, jnp.exp(spread), 0.0)
        scores = dot(q_buf[:, cols], k_buf[:, cols], ((1,), (1,)))
        weighted = (scores * decay).astype(BF16)
        within_buf[:, cols] = dot(weighted, v_buf[:, cols])

    @pl.loop(0, me)
    def _(o):
        pltpu.make_async_remote_copy(
            tots.at[o], tots.at[o], t_send.at[o], t_recv.at[o],
            device_id={"seq": twin}, device_id_type=MESH).wait_recv()

    s_relay()
    s_finish()
    for h in range(heads):
        cols = slice(h * HD, (h + 1) * HD)
        col = run_col_ref[:, h:h + 1]

        def step(o, state):
            return jnp.exp(tots[o, h:h + 1, :]) * state + states[o, cols, :].astype(F32)

        incoming = lax.fori_loop(0, me, step, jnp.zeros((HD, HD), F32))
        carried = dot(
            q_buf[:, cols].astype(F32), incoming, precision=lax.Precision.HIGHEST) * jnp.exp(col)
        raw = within_buf[:, cols] + carried
        ret[:, cols] = (
            raw * lax.rsqrt(jnp.mean(raw * raw, axis=-1, keepdims=True) + 1e-06)).astype(BF16)

    half = width // 2
    piece = half // 3

    def head_copy(src, dst, i, other):
        return pltpu.make_async_remote_copy(
            src, dst, h_send.at[i], h_recv.at[i], device_id={"head": other}, device_id_type=MESH)

    def project(side):
        for c in range(3):
            base = pl.multiple_of(side * half + c * piece, piece)
            term = dot(ret[...], go[pl.ds(base, piece), :], ((1,), (1,)))
            part[side, :, c * piece:(c + 1) * piece] = term.astype(BF16)

    forward(OUT)
    for m in (KEY_GLOBAL, VALUE_GLOBAL, CROSS):
        start_gather(m)
    settle(OUT)
    finish(OUT)
    project(1 - core)
    to_near = head_copy(part.at[1 - core], got_a, 0, near)
    to_near.start()
    project(core)
    to_near.wait_recv()
    pair[...] = (part[core].astype(F32) + got_a[...].astype(F32)).astype(BF16)
    to_far = head_copy(pair, got_b, 1, far)
    to_far.start()
    for m in (KEY_GLOBAL, VALUE_GLOBAL, CROSS):
        forward(m)
    to_far.wait_recv()
    mine[...] = (pair[...].astype(F32) + got_b[...].astype(F32)).astype(BF16)
    back = head_copy(mine, got_c, 2, near)
    back.start()
    for m in (KEY_GLOBAL, VALUE_GLOBAL, CROSS):
        settle(m)
    own_cols = pl.ds(pl.multiple_of(core * half, half), half)
    dec_ref[:, own_cols] = x_ref[:, own_cols].astype(F32) + mine[...].astype(F32)
    back.wait_recv()
    other_cols = pl.ds(pl.multiple_of((1 - core) * half, half), half)
    dec_ref[:, other_cols] = x_ref[:, other_cols].astype(F32) + got_c[...].astype(F32)

    @pl.loop(0, rows // 32)
    def _(i):
        part_rows = pl.ds(i * 32, 32)
        d = dec_ref[part_rows, :]
        normed[part_rows, :] = (
            d * lax.rsqrt(jnp.mean(d * d, axis=-1, keepdims=True) + 1e-06)).astype(BF16)

    dec_copy = pltpu.make_async_copy(dec_ref, dec_out, out_sem)
    dec_copy.start()
    finish(KEY_GLOBAL)
    finish(VALUE_GLOBAL)
    kvs[me, :, :HD] = dot(normed[...], gkg[...]).astype(BF16)
    kvs[me, :, HD:] = dot(normed[...], gvg[...]).astype(BF16)
    kv_start, kv_relay, kv_finish, kv_done = causal_ops(kvs, kv_send, kv_recv, kvx_send)
    kv_start()
    finish(CROSS)
    cross = (dot(normed[...], gc[...]) * HD ** -0.5).astype(BF16)
    for g in range(heads):
        q_rows[g * rows:(g + 1) * rows, :] = cross[:, g * HD:(g + 1) * HD]

    for g in range(heads):
        block = slice(g * rows, (g + 1) * rows)
        scores = dot(q_rows[block, :], kvs[me, :, :HD], ((1,), (1,)))
        scores = jnp.where(t_iota >= s_iota, scores, -1e30)
        high = jnp.max(scores, axis=-1, keepdims=True)
        weights = jnp.exp(scores - high)
        top[block, :] = high
        total[block, :] = jnp.sum(weights, axis=-1, keepdims=True)
        acc[block, :] = dot(weights.astype(BF16), kvs[me, :, HD:])

    def attend(o):
        for g in range(heads):
            block = slice(g * rows, (g + 1) * rows)
            scores = dot(q_rows[block, :], kvs[o, :, :HD], ((1,), (1,)))
            old = top[block, :]
            high = jnp.maximum(old, jnp.max(scores, axis=-1, keepdims=True))
            weights = jnp.exp(scores - high)
            shrink = jnp.exp(old - high)
            top[block, :] = high
            total[block, :] = total[block, :] * shrink + jnp.sum(weights, axis=-1, keepdims=True)
            acc[block, :] = acc[block, :] * shrink + dot(weights.astype(BF16), kvs[o, :, HD:])

    kv_relay(attend)
    kv_finish(attend)

    for g in range(heads):
        block = slice(g * rows, (g + 1) * rows)
        att_ref[:, g * HD:(g + 1) * HD] = (acc[block, :] / total[block, :]).astype(BF16)

    @pl.loop(me + 1, n)
    def _(p):
        total_copy(p).wait_send()

    for m in range(7):
        finish_sends(m)
    tokens.wait_send()
    for m in range(3):
        twin_copy(sent.at[m], got.at[m], m).wait_send()
    dec_copy.wait()
    s_done()
    kv_done()
    to_near.wait_send()
    to_far.wait_send()
    back.wait_send()


def body(n, inputs, decay_logs, wq, wk, wv, wo, kg, vg, qc):
    rows, width = inputs.shape
    inner = wq.shape[1]
    heads = inner // HD
    running = jnp.cumsum(decay_logs, axis=-1)
    run_row = jnp.pad(running, ((0, 8 - heads), (0, 0)))
    run_col = run_row.T
    totals = jnp.broadcast_to(run_row[:, -1:], (8, HD))
    depth = wq.shape[0]
    aligned = depth % HD == 0
    half_n = n // 2
    half = width // 2
    small = inputs[:16, :HD].reshape(1, 16, HD)
    split = inputs.reshape(rows, half_n, 2, depth).transpose(2, 0, 1, 3).reshape(2, rows, half)
    vmem = pl.BlockSpec(memory_space=pltpu.VMEM)
    dma = pltpu.SemaphoreType.DMA
    mid = max(half_n // 2, 1)
    return pl.pallas_call(
        functools.partial(kernel, n, aligned),
        out_shape=(
            jax.ShapeDtypeStruct((rows, width), F32),
            jax.ShapeDtypeStruct((rows, inner), BF16),
        ),
        in_specs=[vmem] * 12,
        out_specs=(pl.BlockSpec(memory_space=pl.ANY), vmem),
        scratch_shapes=[
            pltpu.VMEM((half, inner), BF16),
            pltpu.VMEM((half, inner), BF16),
            pltpu.VMEM((half, inner), BF16),
            pltpu.VMEM((width, inner), BF16),
            pltpu.VMEM((width, inner), BF16),
            pltpu.VMEM((width, HD), BF16),
            pltpu.VMEM((width, HD), BF16),
            pltpu.VMEM((n, 8, HD), F32),
            pltpu.VMEM((n, inner, HD), BF16),
            pltpu.VMEM((n, rows, 2 * HD), BF16),
            pltpu.VMEM((rows, width), F32),
            pltpu.VMEM((2, rows, half), BF16),
            pltpu.VMEM((rows, half), BF16),
            pltpu.VMEM((3, rows, inner), BF16),
            pltpu.VMEM((3, rows, inner), BF16),
            pltpu.VMEM((rows, inner), F32),
            pltpu.VMEM((rows, width), BF16),
            pltpu.VMEM((rows, inner), BF16),
            pltpu.VMEM((rows, inner), BF16),
            pltpu.VMEM((rows, inner), BF16),
            pltpu.VMEM((rows, inner), BF16),
            pltpu.VMEM((2, rows, half), BF16),
            pltpu.VMEM((rows, half), BF16),
            pltpu.VMEM((rows, half), BF16),
            pltpu.VMEM((rows, half), BF16),
            pltpu.VMEM((rows, half), BF16),
            pltpu.VMEM((rows, half), BF16),
            pltpu.VMEM((heads * rows, HD), BF16),
            pltpu.VMEM((heads * rows, 1), F32),
            pltpu.VMEM((heads * rows, 1), F32),
            pltpu.VMEM((heads * rows, HD), F32),
            dma((7, mid)), dma((7, mid)), dma((7, n)), dma((7, half_n)), dma((7,)),
            dma((n,)), dma((n,)),
            dma((half_n,)), dma((n,)), dma((half_n,)),
            dma((half_n,)), dma((n,)), dma((half_n,)),
            dma((3,)), dma((3,)), dma((4,)), dma((4,)), dma,
        ],
        compiler_params=pltpu.CompilerParams(
            collective_id=0, has_side_effects=True, vmem_limit_bytes=62 * 1024 * 1024),
        name="layer",
    )(inputs, small if aligned else split, run_row, run_col, totals, wk, wv, wq, wo, qc, kg, vg)


def solution(mesh):
    n = mesh.shape["seq"]

    def run(*args):
        return body(n, *args)

    in_specs = (P("seq", None), P("head", "seq")) + (P("seq", "head"),) * 7
    out_specs = (P("seq", None), P("seq", "head"))
    return jax.shard_map(run, mesh=mesh, in_specs=in_specs, out_specs=out_specs, check_vma=False)
```
